32 devices in a mesh: mem: 4 (over x, core), slab: 8 (over z, y).
Axes of the slice: x: 2, y: 2, z: 4, core: 2. Of those that a mesh axis runs over, the one named last changes fastest.
Arguments:
- anomalies: bfloat16 [8, 4096, 4096], P('mem', 'slab'), may hold values from -2.390625 to 2.390625
- increment: float32 [4096, 4096], P('slab'), may hold values from -6 to 6
- spectrum: float32 [4096, 4096], P(None, 'slab'), may hold values from 0.01 to 2, as said below
Outputs:
- product: float32 [4096, 4096], P('slab')
The draws below stay inside these ranges and needn't reach their ends.
Inputs may be any that keep to these rules, and one draw needn't show every extreme that they name: spectrum[k, l] equals spectrum[(4096 - k) % 4096, (4096 - l) % 4096], and is positive.
All inputs are finite; a program needn't handle non-finite values.
Results may differ from the reference program's by a relative error of at most 0.0003.
Values sent between devices are 32-bit elements; how exact they have to be, the bound alone decides.
No kernel may reach another device: no remote copies, remote signals or barrier semaphores. Data moves between devices by JAX's collectives and lax.ppermute only.
A program may use at most 192 MiB of HBM per device.

```python
import jax
import jax.numpy as jnp
from jax import lax

NX = 4096
NY = 4096
MEMBERS = 8


def draw_spectrum(key, part):
    logs = jax.random.uniform(key, (NX, NY), jnp.float32, jnp.log(0.05), 0.0)
    values = jnp.exp(logs)
    mirrored = jnp.roll(jnp.flip(values, (0, 1)), 1, (0, 1))
    result = 0.5 * (values + mirrored)
    return result


def shard_levels(own_key, extent, split, low, top_value):
    loudness, own = 1.0, jax.random.fold_in(own_key, 6)
    for dim, shards_of in split:
        steps = jnp.exp(jax.random.uniform(jax.random.fold_in(own, dim), (shards_of,), jnp.float32, low / len(split), top_value / len(split)))
        loudness = loudness * jnp.repeat(steps, extent[dim] // shards_of).reshape([-1 if axis == dim else 1 for axis in range(len(extent))])
    return loudness


def noise(key, shape, spread, limit, pieces=(), held_as=jnp.bfloat16):
    level = shard_levels(key, shape, pieces, -0.22, 0.18) if pieces else 1.0
    array = jax.random.normal(key, shape, jnp.float32) * spread * level
    return jnp.minimum(jnp.maximum(array, -limit), limit).astype(held_as)


def setup_inputs(seed: int = 0) -> dict:
    streams_of = jax.random.split(jax.random.key(seed), 4)
    anomalies = noise(streams_of[0], (MEMBERS, NX, NY), 0.4, 2.390625, ((0, 4), (1, 8)))
    increment = noise(streams_of[1], (NX, NY), 1.0, 6.0, ((0, 8),), jnp.float32)
    spectrum = draw_spectrum(jax.random.fold_in(streams_of[3], 71), 0)
    return {"anomalies": anomalies, "increment": increment, "spectrum": spectrum}


def reference(anomalies, increment, spectrum):
    def member_term(index, total):
        member = lax.dynamic_index_in_dim(anomalies, index, 0, keepdims=False).astype(jnp.float32)
        field = member * increment
        waves = jnp.fft.fft2(field)
        filtered = jnp.real(jnp.fft.ifft2(waves * spectrum))
        return total + member * filtered

    start = jnp.zeros((NX, NY), jnp.float32)
    return lax.fori_loop(0, MEMBERS, member_term, start)
```

```python
import math

import jax
import jax.numpy as jnp
from jax import lax
from jax.sharding import PartitionSpec as P

CHUNKS = 2


def section_table(length, sign):
    index = jnp.arange(length, dtype=jnp.int32)
    angle = 2.0 * math.pi / length * (index[:, None] * index[None, :] % length).astype(jnp.float32)
    cos, sin = jnp.cos(angle), sign * jnp.sin(angle)
    return jnp.stack([jnp.stack([cos, sin], 1), jnp.stack([-sin, cos], 1)], 0)


def dft_tables(length, sign):
    first = 1 << (length.bit_length() - 1) // 2
    second = length // first
    index_a = jnp.arange(first, dtype=jnp.int32)
    index_b = jnp.arange(second, dtype=jnp.int32)
    angle = (
        2.0 * math.pi / length * (index_a[:, None] * index_b[None, :] % length).astype(jnp.float32)
    )
    twist = (jnp.cos(angle)[:, :, None], sign * jnp.sin(angle)[:, :, None])
    return first, second, section_table(first, sign), twist, section_table(second, sign)


def transform(parts, factors):
    first, second, table_one, (tw_cos, tw_sin), table_two = factors
    high = lax.Precision.HIGH
    cut = parts.reshape(2, first, second, parts.shape[2])
    step = jnp.einsum("pabk,paqc->qcbk", cut, table_one, precision=high)
    twisted = jnp.stack(
        [step[0] * tw_cos - step[1] * tw_sin, step[0] * tw_sin + step[1] * tw_cos], 0
    )
    return jnp.einsum("pcbk,pbqd->qdck", twisted, table_two, precision=high).reshape(parts.shape)


def per_device(anomalies, increment, spectrum, slabs):
    pairs, row_count, col_count = anomalies.shape[0] // 2, anomalies.shape[1], anomalies.shape[2]
    row_total, own_cols = spectrum.shape
    forward_y = dft_tables(col_count, -1.0)
    inverse_y = dft_tables(col_count, 1.0)
    forward_x = dft_tables(row_total, -1.0)
    inverse_x = dft_tables(row_total, 1.0)
    scaled = spectrum * (1.0 / (row_total * col_count))
    total = jnp.zeros_like(increment)
    width = own_cols // CHUNKS
    for pair in range(pairs):
        members = anomalies[2 * pair : 2 * pair + 2].astype(jnp.float32)
        fields = jnp.swapaxes(members * increment[None], 1, 2)
        waves = transform(fields, forward_y).reshape(2, slabs, own_cols, row_count)
        backs = []
        for chunk in range(CHUNKS):
            own = slice(chunk * width, (chunk + 1) * width)
            sent = lax.all_to_all(
                waves[:, :, own, :], "slab", split_axis=1, concat_axis=1, tiled=True
            )
            cols = sent.transpose(0, 1, 3, 2).reshape(2, row_total, width)
            cols = transform(cols, forward_x) * scaled[None, :, own]
            cols = transform(cols, inverse_x).reshape(2, slabs, row_count, width)
            back = cols.transpose(0, 1, 3, 2)
            backs.append(lax.all_to_all(back, "slab", split_axis=1, concat_axis=1, tiled=True))
        rows = jnp.concatenate(backs, 2).reshape(2, col_count, row_count)
        filtered = jnp.swapaxes(transform(rows, inverse_y), 1, 2)
        total = total + members[0] * filtered[0] + members[1] * filtered[1]
    return lax.psum(total, "mem")


def solution(mesh):
    placed = (P("mem", "slab", None), P("slab", None), P(None, "slab"))

    def body(anomalies, increment, spectrum):
        return per_device(anomalies, increment, spectrum, mesh.shape["slab"])

    return jax.shard_map(
        body, mesh=mesh, in_specs=placed, out_specs=P("slab", None), check_vma=False
    )
```
